32 devices in a mesh: expert: 16 (over z, y, core), tensor: 2 (over x).
Axes of the slice: x: 2, y: 2, z: 4, core: 2. Of those that a mesh axis runs over, the one named last changes fastest.
Arguments:
- tokens: bfloat16 [64, 256, 1280], P(('expert', 'tensor')), may hold values from -6 to 6
- slot_keys: bfloat16 [1280, 16], replicated, may hold values from -6 to 6
- logit_scale: float32 [], replicated, may hold values from 40 to 80
- w_in: bfloat16 [16, 1280, 3584], P('expert', None, 'tensor'), may hold values from -0.625 to 0.625
- b_in: bfloat16 [16, 3584], P('expert', 'tensor'), may hold values from -3 to 3
- w_out: bfloat16 [16, 3584, 1280], P('expert', 'tensor'), may hold values from -0.09375 to 0.09375
- b_out: bfloat16 [16, 1280], P('expert'), may hold values from -3 to 3
Outputs:
- mixed: bfloat16 [64, 256, 1280], P(('expert', 'tensor'))
The draws below stay inside these ranges and needn't reach their ends.
All inputs are finite; a program needn't handle non-finite values.
Results may differ from the reference program's by a relative error of at most 0.0071.
Values may be sent and summed in bfloat16 or wider, within the bound.
A program may use at most 64 MiB of HBM per device.

```python
import math
import jax
import jax.numpy as jnp
from jax import lax

D = 1280
FF = 3584
SEQ = 256
EXPERTS = 16
IMAGES = 64


def shard_levels(key, shape, split, smallest, top_value):
    factor_of, own = 1.0, jax.random.fold_in(key, 6)
    for position, shards_of in split:
        heights = jnp.exp(jax.random.uniform(jax.random.fold_in(own, position), (shards_of,), jnp.float32, smallest / len(split), top_value / len(split)))
        factor_of = factor_of * jnp.repeat(heights, shape[position] // shards_of).reshape([-1 if axis == position else 1 for axis in range(len(shape))])
    return factor_of


def noise(own_key, dims, width, limit, pieces=(), held_as=jnp.bfloat16):
    values = width * jax.random.normal(own_key, dims, jnp.float32)
    if pieces:
        values = values * shard_levels(own_key, dims, pieces, -0.22, 0.18)
    return jnp.clip(values, -limit, limit).astype(held_as)


def setup_inputs(seed: int = 0) -> dict:
    streams_of = jax.random.split(jax.random.key(seed), 8)
    tokens = noise(streams_of[0], (IMAGES, SEQ, D), 1.0, 6.0, ((0, 32),))
    slot_keys = noise(streams_of[1], (D, EXPERTS), 1.0, 6.0)
    logit_scale = jnp.clip(jnp.exp(jax.random.uniform(streams_of[2], (), jnp.float32, math.log(40.0), math.log(80.0))), 40.0, 80.0)
    w_in = noise(streams_of[3], (EXPERTS, D, FF), (D // 16) ** -0.5, 0.625, ((0, 16), (2, 2)))
    b_in = noise(streams_of[4], (EXPERTS, FF), 0.5, 3.0, ((0, 16), (1, 2)))
    w_out = noise(streams_of[5], (EXPERTS, FF, D), FF ** -0.5, 0.09375, ((0, 16), (1, 2)))
    b_out = noise(streams_of[6], (EXPERTS, D), 0.5, 3.0, ((0, 16),))
    return {"tokens": tokens, "slot_keys": slot_keys, "logit_scale": logit_scale, "w_in": w_in, "b_in": b_in, "w_out": w_out, "b_out": b_out}


EPS = 1e-06

def expert_apply(args):
    slot_rows, weight_in, bias_in, weight_out, bias_out = args
    pre = jnp.dot(slot_rows, weight_in, preferred_element_type=jnp.float32) + bias_in.astype(jnp.float32)
    hidden = jax.nn.gelu(pre).astype(jnp.bfloat16)
    result = jnp.dot(hidden, weight_out, preferred_element_type=jnp.float32) + bias_out.astype(jnp.float32)
    return result.astype(jnp.bfloat16)

def reference(tokens, slot_keys, logit_scale, w_in, b_in, w_out, b_out):
    tok_wide = tokens.astype(jnp.float32)
    key_wide = slot_keys.astype(jnp.float32)
    row_inv = lax.rsqrt(lax.optimization_barrier(jnp.sum(tok_wide * tok_wide, axis=2, keepdims=True)) + EPS)
    key_inv = lax.rsqrt(lax.optimization_barrier(jnp.sum(key_wide * key_wide, axis=0)) + EPS)
    raw = jnp.einsum('imd,ds->ims', tok_wide, key_wide)
    logits = logit_scale * row_inv * key_inv * raw
    expo = jnp.exp(logits)
    dispatch = (expo / lax.optimization_barrier(jnp.sum(expo, axis=1, keepdims=True))).astype(jnp.bfloat16)
    combine = (expo / lax.optimization_barrier(jnp.sum(expo, axis=2, keepdims=True))).astype(jnp.bfloat16)
    slot_in = jnp.einsum('ims,imd->sid', dispatch.astype(jnp.float32), tok_wide).astype(jnp.bfloat16)
    slot_out = lax.map(expert_apply, (slot_in, w_in, b_in, w_out, b_out))
    mixed = jnp.einsum('ims,sid->imd', combine.astype(jnp.float32), slot_out.astype(jnp.float32))
    return mixed.astype(jnp.bfloat16)
```

```python
import functools

import jax
import jax.numpy as jnp
from jax import lax
from jax.experimental import pallas as pl
from jax.experimental.pallas import tpu as pltpu
from jax.sharding import PartitionSpec as P

EPS = 1e-06
MESH = pl.DeviceIdType.MESH
NT = (((1,), (1,)), ((), ()))


def column_cuts(width):
    first = (width * 3 // 5) // 256 * 256
    return [(0, first), (first, width - first)] if 0 < first < width else [(0, width)]


def kernel(
    experts, tensors, cuts,
    tokens_hbm, keys_ref, scale_ref, w_in_hbm, b_in_ref, w_out_hbm, b_out_ref,
    out_ref,
    tok, w_in, w_out, send1, recv1, x2, hidden, comb, *rest,
):
    n_cut = len(cuts)
    send2, recv2 = rest[:n_cut], rest[n_cut:2 * n_cut]
    load_sem, send_sem1, recv_sem1, send_sem2, recv_sem2 = rest[2 * n_cut:]
    images, seq, width = tok.shape
    slots = keys_ref.shape[1]
    rows = slots * images
    devices = experts * tensors
    e, t = lax.axis_index("expert"), lax.axis_index("tensor")
    me = e * tensors + t
    home = t * experts + e

    loads = [
        pltpu.make_async_copy(tokens_hbm, tok, load_sem.at[0]),
        pltpu.make_async_copy(w_in_hbm.at[0], w_in, load_sem.at[1]),
        pltpu.make_async_copy(w_out_hbm.at[0], w_out, load_sem.at[2]),
    ]
    for load in loads:
        load.start()

    def peer(step):
        j = lax.rem(me + step, devices)
        je, jt = j // tensors, lax.rem(j, tensors)
        return j, je, {"expert": je, "tensor": jt}

    barrier = pltpu.get_barrier_semaphore()

    @pl.loop(1, devices)
    def _(step):
        pl.semaphore_signal(barrier, inc=1, device_id=peer(step)[2], device_id_type=MESH)

    row_slot = lax.broadcasted_iota(jnp.int32, (rows, slots), 0) // images
    col_slot = lax.broadcasted_iota(jnp.int32, (rows, slots), 1)
    spread = jnp.where(row_slot == col_slot, 1.0, 0.0).astype(jnp.bfloat16)
    keys_t = lax.dot_general(spread, keys_ref[...], NT, preferred_element_type=jnp.float32)
    key_inv = lax.rsqrt(jnp.sum(keys_t * keys_t, axis=1, keepdims=True) + EPS)
    key_gain = key_inv * scale_ref[0]
    keys_b = keys_t.astype(jnp.bfloat16)

    loads[0].wait()
    flat = tok[...].reshape(images * seq, width)
    raw = lax.dot_general(keys_b, flat, NT, preferred_element_type=jnp.float32)
    part = jnp.zeros((images * seq, 128), jnp.float32)
    for c in range(width // 128):
        piece = flat[:, c * 128:(c + 1) * 128].astype(jnp.float32)
        part = part + piece * piece
    row_sq = lax.dot_general(
        jnp.ones((8, 128), jnp.float32), part, NT,
        precision=lax.Precision.HIGHEST, preferred_element_type=jnp.float32,
    )[0:1]
    logits = key_gain * lax.rsqrt(row_sq + EPS) * raw
    row_image = lax.broadcasted_iota(jnp.int32, logits.shape, 0) % images
    col_image = lax.broadcasted_iota(jnp.int32, logits.shape, 1) // seq
    expo = jnp.where(row_image == col_image, jnp.exp(logits), 0.0)
    dispatch = (expo / jnp.sum(expo, axis=1, keepdims=True)).astype(jnp.bfloat16)
    slot_in = jnp.dot(dispatch, flat, preferred_element_type=jnp.float32).astype(jnp.bfloat16)
    for s in range(slots):
        send1[s] = slot_in[s * images:(s + 1) * images]

    pl.semaphore_wait(barrier, devices - 1)

    own = pltpu.make_async_copy(send1.at[e], recv1.at[me], recv_sem1)
    own.start()

    @pl.loop(1, devices)
    def _(step):
        _, je, device = peer(step)
        pltpu.make_async_remote_copy(
            src_ref=send1.at[je], dst_ref=recv1.at[me], send_sem=send_sem1, recv_sem=recv_sem1,
            device_id=device, device_id_type=MESH,
        ).start()

    combine = expo / jnp.sum(expo, axis=0, keepdims=True)
    comb[...] = jnp.concatenate([combine] * tensors, axis=0).T.astype(jnp.bfloat16)

    loads[1].wait()
    pltpu.make_async_copy(recv1, recv1, recv_sem1).wait()
    for k in range(devices):
        x2[k * images:(k + 1) * images, :] = recv1[k]
    x = x2[...]
    half = w_in.shape[1]
    for c in range(0, half, 256):
        size = min(256, half - c)
        pre = jnp.dot(x, w_in[:, c:c + size], preferred_element_type=jnp.float32)
        pre = pre + b_in_ref[:, c:c + size].astype(jnp.float32)
        hidden[:, c:c + size] = jax.nn.gelu(pre).astype(jnp.bfloat16)

    loads[2].wait()
    h = hidden[...]
    first_half = jnp.where(t == 0, 1.0, 0.0)
    for c, (start, size) in enumerate(cuts):
        y = jnp.dot(h, w_out[:, start:start + size], preferred_element_type=jnp.float32)
        y = y + b_out_ref[:, start:start + size].astype(jnp.float32) * first_half
        y = y.astype(jnp.bfloat16)
        for k in range(devices):
            send2[c][k] = y[k * images:(k + 1) * images]
        pltpu.make_async_copy(send2[c].at[me], recv2[c].at[home], recv_sem2.at[c]).start()

        @pl.loop(1, devices)
        def _(step):
            j, _, device = peer(step)
            pltpu.make_async_remote_copy(
                src_ref=send2[c].at[j], dst_ref=recv2[c].at[home],
                send_sem=send_sem2.at[c], recv_sem=recv_sem2.at[c],
                device_id=device, device_id_type=MESH,
            ).start()

    cm = comb[...]
    for c, (start, size) in enumerate(cuts):
        pltpu.make_async_copy(recv2[c], recv2[c], recv_sem2.at[c]).wait()
        for k in range(devices):
            x2[k * images:(k + 1) * images, start:start + size] = recv2[c][k]
        mixed = jnp.dot(cm, x2[:, start:start + size], preferred_element_type=jnp.float32)
        out_ref[:, :, start:start + size] = mixed.astype(jnp.bfloat16).reshape(images, seq, size)

    first = recv1.at[pl.ds(0, devices - 1)]
    pltpu.make_async_copy(first, first, send_sem1).wait()
    for c in range(n_cut):
        block = recv2[c].at[pl.ds(0, devices - 1)]
        pltpu.make_async_copy(block, block, send_sem2.at[c]).wait()


def local(experts, tensors, tokens, slot_keys, logit_scale, w_in, b_in, w_out, b_out):
    images, seq, width = tokens.shape
    slots = slot_keys.shape[1]
    half = w_in.shape[2]
    devices = experts * tensors
    cuts = column_cuts(width)
    bf16 = jnp.bfloat16
    return pl.pallas_call(
        functools.partial(kernel, experts, tensors, cuts),
        out_shape=jax.ShapeDtypeStruct(tokens.shape, bf16),
        in_specs=[
            pl.BlockSpec(memory_space=pl.ANY),
            pl.BlockSpec(memory_space=pltpu.VMEM),
            pl.BlockSpec(memory_space=pltpu.SMEM),
            pl.BlockSpec(memory_space=pl.ANY),
            pl.BlockSpec(memory_space=pltpu.VMEM),
            pl.BlockSpec(memory_space=pl.ANY),
            pl.BlockSpec(memory_space=pltpu.VMEM),
        ],
        out_specs=pl.BlockSpec(memory_space=pltpu.VMEM),
        scratch_shapes=[
            pltpu.VMEM((images, seq, width), bf16),
            pltpu.VMEM((width, half), bf16),
            pltpu.VMEM((half, width), bf16),
            pltpu.VMEM((slots, images, width), bf16),
            pltpu.VMEM((devices, images, width), bf16),
            pltpu.VMEM((devices * images, width), bf16),
            pltpu.VMEM((devices * images, half), bf16),
            pltpu.VMEM((images * seq, tensors * slots * images), bf16),
            *[pltpu.VMEM((devices, images, size), bf16) for _, size in cuts],
            *[pltpu.VMEM((devices, images, size), bf16) for _, size in cuts],
            pltpu.SemaphoreType.DMA((3,)),
            pltpu.SemaphoreType.DMA,
            pltpu.SemaphoreType.DMA,
            pltpu.SemaphoreType.DMA((len(cuts),)),
            pltpu.SemaphoreType.DMA((len(cuts),)),
        ],
        compiler_params=pltpu.CompilerParams(collective_id=0, has_side_effects=True),
    )(tokens, slot_keys, logit_scale.reshape(1), w_in, b_in, w_out, b_out)


def solution(mesh):
    placed = (
        P(("expert", "tensor"), None, None),
        P(),
        P(),
        P("expert", None, "tensor"),
        P("expert", "tensor"),
        P("expert", "tensor", None),
        P("expert", None),
    )
    return jax.shard_map(
        functools.partial(local, mesh.shape["expert"], mesh.shape["tensor"]),
        mesh=mesh,
        in_specs=placed,
        out_specs=P(("expert", "tensor"), None, None),
        check_vma=False,
    )
```

```python
import functools

import jax
import jax.numpy as jnp
from jax import lax
from jax.experimental import pallas as pl
from jax.experimental.pallas import tpu as pltpu
from jax.sharding import PartitionSpec as P

EPS = 1e-06
MESH = pl.DeviceIdType.MESH
NT = (((1,), (1,)), ((), ()))


def column_cuts(width):
    first = (width * 3 // 5) // 256 * 256
    return [(0, first), (first, width - first)] if 0 < first < width else [(0, width)]


def kernel(
    experts, tensors, cuts,
    tokens_hbm, keys_ref, scale_ref, w_in_hbm, b_in_ref, w_out_hbm, b_out_ref,
    out_ref,
    tok, w_in, w_out, send1, recv1, x2, hidden, comb, *rest,
):
    n_cut = len(cuts)
    send2, recv2 = rest[:n_cut], rest[n_cut:2 * n_cut]
    load_sem, send_sem1, recv_sem1, send_sem2, recv_sem2 = rest[2 * n_cut:]
    images, seq, width = tok.shape
    slots = keys_ref.shape[0]
    rows = slots * images
    devices = experts * tensors
    e, t = lax.axis_index("expert"), lax.axis_index("tensor")
    me = e * tensors + t
    home = t * experts + e

    loads = [
        pltpu.make_async_copy(tokens_hbm, tok, load_sem.at[0]),
        pltpu.make_async_copy(w_in_hbm.at[0], w_in, load_sem.at[1]),
        pltpu.make_async_copy(w_out_hbm.at[0], w_out, load_sem.at[2]),
    ]
    for load in loads:
        load.start()

    def peer(step):
        j = lax.rem(me + step, devices)
        je, jt = j // tensors, lax.rem(j, tensors)
        return j, je, {"expert": je, "tensor": jt}

    barrier = pltpu.get_barrier_semaphore()

    @pl.loop(1, devices)
    def _(step):
        pl.semaphore_signal(barrier, inc=1, device_id=peer(step)[2], device_id_type=MESH)

    row_slot = lax.broadcasted_iota(jnp.int32, (rows, slots), 0) // images
    col_slot = lax.broadcasted_iota(jnp.int32, (rows, slots), 1)
    spread = jnp.where(row_slot == col_slot, 1.0, 0.0).astype(jnp.bfloat16)
    keys_t = jnp.dot(spread, keys_ref[...], preferred_element_type=jnp.float32)
    key_inv = lax.rsqrt(jnp.sum(keys_t * keys_t, axis=1, keepdims=True) + EPS)
    key_gain = key_inv * scale_ref[0]
    keys_b = keys_t.astype(jnp.bfloat16)

    loads[0].wait()
    flat = tok[...].reshape(images * seq, width)
    raw = lax.dot_general(keys_b, flat, NT, preferred_element_type=jnp.float32)
    part = jnp.zeros((images * seq, 128), jnp.float32)
    for c in range(width // 128):
        piece = flat[:, c * 128:(c + 1) * 128].astype(jnp.float32)
        part = part + piece * piece
    row_sq = lax.dot_general(
        jnp.ones((8, 128), jnp.float32), part, NT,
        precision=lax.Precision.HIGHEST, preferred_element_type=jnp.float32,
    )[0:1]
    logits = key_gain * lax.rsqrt(row_sq + EPS) * raw
    row_image = lax.broadcasted_iota(jnp.int32, logits.shape, 0) % images
    col_image = lax.broadcasted_iota(jnp.int32, logits.shape, 1) // seq
    expo = jnp.where(row_image == col_image, jnp.exp(logits), 0.0)
    dispatch = (expo / jnp.sum(expo, axis=1, keepdims=True)).astype(jnp.bfloat16)
    slot_in = jnp.dot(dispatch, flat, preferred_element_type=jnp.float32).astype(jnp.bfloat16)
    for s in range(slots):
        send1[s] = slot_in[s * images:(s + 1) * images]

    pl.semaphore_wait(barrier, devices - 1)

    own = pltpu.make_async_copy(send1.at[e], recv1.at[me], recv_sem1)
    own.start()

    @pl.loop(1, devices)
    def _(step):
        _, je, device = peer(step)
        pltpu.make_async_remote_copy(
            src_ref=send1.at[je], dst_ref=recv1.at[me], send_sem=send_sem1, recv_sem=recv_sem1,
            device_id=device, device_id_type=MESH,
        ).start()

    combine = expo / jnp.sum(expo, axis=0, keepdims=True)
    comb[...] = jnp.concatenate([combine] * tensors, axis=0).T.astype(jnp.bfloat16)

    loads[1].wait()
    pltpu.make_async_copy(recv1, recv1, recv_sem1).wait()
    for k in range(devices):
        x2[k * images:(k + 1) * images, :] = recv1[k]
    x = x2[...]
    half = w_in.shape[1]
    for c in range(0, half, 256):
        size = min(256, half - c)
        pre = jnp.dot(x, w_in[:, c:c + size], preferred_element_type=jnp.float32)
        pre = pre + b_in_ref[:, c:c + size].astype(jnp.float32)
        hidden[:, c:c + size] = jax.nn.gelu(pre).astype(jnp.bfloat16)

    loads[2].wait()
    h = hidden[...]
    first_half = jnp.where(t == 0, 1.0, 0.0)
    for c, (start, size) in enumerate(cuts):
        y = jnp.dot(h, w_out[:, start:start + size], preferred_element_type=jnp.float32)
        y = y + b_out_ref[:, start:start + size].astype(jnp.float32) * first_half
        y = y.astype(jnp.bfloat16)
        for k in range(devices):
            send2[c][k] = y[k * images:(k + 1) * images]
        pltpu.make_async_copy(send2[c].at[me], recv2[c].at[home], recv_sem2.at[c]).start()

        @pl.loop(1, devices)
        def _(step):
            j, _, device = peer(step)
            pltpu.make_async_remote_copy(
                src_ref=send2[c].at[j], dst_ref=recv2[c].at[home],
                send_sem=send_sem2.at[c], recv_sem=recv_sem2.at[c],
                device_id=device, device_id_type=MESH,
            ).start()

    cm = comb[...]
    for c, (start, size) in enumerate(cuts):
        pltpu.make_async_copy(recv2[c], recv2[c], recv_sem2.at[c]).wait()
        for k in range(devices):
            x2[k * images:(k + 1) * images, start:start + size] = recv2[c][k]
        mixed = jnp.dot(cm, x2[:, start:start + size], preferred_element_type=jnp.float32)
        out_ref[:, :, start:start + size] = mixed.astype(jnp.bfloat16).reshape(images, seq, size)

    first = recv1.at[pl.ds(0, devices - 1)]
    pltpu.make_async_copy(first, first, send_sem1).wait()
    for c in range(n_cut):
        block = recv2[c].at[pl.ds(0, devices - 1)]
        pltpu.make_async_copy(block, block, send_sem2.at[c]).wait()


def local(experts, tensors, tokens, slot_keys, logit_scale, w_in, b_in, w_out, b_out):
    images, seq, width = tokens.shape
    slots = slot_keys.shape[1]
    half = w_in.shape[2]
    devices = experts * tensors
    cuts = column_cuts(width)
    bf16 = jnp.bfloat16
    return pl.pallas_call(
        functools.partial(kernel, experts, tensors, cuts),
        out_shape=pltpu.VMEM(tokens.shape, bf16),
        in_specs=[
            pl.BlockSpec(memory_space=pltpu.HBM),
            pl.BlockSpec(memory_space=pltpu.VMEM),
            pl.BlockSpec(memory_space=pltpu.SMEM),
            pl.BlockSpec(memory_space=pltpu.HBM),
            pl.BlockSpec(memory_space=pltpu.VMEM),
            pl.BlockSpec(memory_space=pltpu.HBM),
            pl.BlockSpec(memory_space=pltpu.VMEM),
        ],
        out_specs=pl.BlockSpec(memory_space=pltpu.VMEM),
        scratch_shapes=[
            pltpu.VMEM((images, seq, width), bf16),
            pltpu.VMEM((width, half), bf16),
            pltpu.VMEM((half, width), bf16),
            pltpu.VMEM((slots, images, width), bf16),
            pltpu.VMEM((devices, images, width), bf16),
            pltpu.VMEM((devices * images, width), bf16),
            pltpu.VMEM((devices * images, half), bf16),
            pltpu.VMEM((images * seq, tensors * slots * images), bf16),
            *[pltpu.VMEM((devices, images, size), bf16) for _, size in cuts],
            *[pltpu.VMEM((devices, images, size), bf16) for _, size in cuts],
            pltpu.SemaphoreType.DMA((3,)),
            pltpu.SemaphoreType.DMA,
            pltpu.SemaphoreType.DMA,
            pltpu.SemaphoreType.DMA((len(cuts),)),
            pltpu.SemaphoreType.DMA((len(cuts),)),
        ],
        compiler_params=pltpu.CompilerParams(collective_id=0, has_side_effects=True, vmem_limit_bytes=61 * 2**20),
    )(tokens, slot_keys.T, logit_scale.reshape(1), w_in, b_in, w_out, b_out)


def solution(mesh):
    placed = (
        P(("expert", "tensor"), None, None),
        P(),
        P(),
        P("expert", None, "tensor"),
        P("expert", "tensor"),
        P("expert", "tensor", None),
        P("expert", None),
    )
    return jax.shard_map(
        functools.partial(local, mesh.shape["expert"], mesh.shape["tensor"]),
        mesh=mesh,
        in_specs=placed,
        out_specs=P(("expert", "tensor"), None, None),
        check_vma=False,
    )
```

```python
import functools

import jax
import jax.numpy as jnp
from jax import lax
from jax.experimental import pallas as pl
from jax.experimental.pallas import tpu as pltpu
from jax.sharding import PartitionSpec as P

EPS = 1e-06
MESH = pl.DeviceIdType.MESH
NT = (((1,), (1,)), ((), ()))


def kernel(
    experts, tensors, cuts,
    tokens_hbm, keys_ref, scale_ref, w_in_hbm, b_in_ref, w_out_hbm, b_out_ref,
    out_ref,
    tok, w_in, w_out, send1, recv1, x2, hidden, comb, *rest,
):
    n_cut = len(cuts)
    send2, recv2 = rest[:n_cut], rest[n_cut:2 * n_cut]
    load_sem, send_sem1, recv_sem1, send_sem2, recv_sem2 = rest[2 * n_cut:]
    images, seq, width = tok.shape
    slots = keys_ref.shape[0]
    rows = slots * images
    devices = experts * tensors
    e, t = lax.axis_index("expert"), lax.axis_index("tensor")
    me = e * tensors + t
    home = t * experts + e

    loads = [
        pltpu.make_async_copy(tokens_hbm, tok, load_sem.at[0]),
        pltpu.make_async_copy(w_in_hbm.at[0], w_in, load_sem.at[1]),
        pltpu.make_async_copy(w_out_hbm.at[0], w_out, load_sem.at[2]),
    ]
    for load in loads:
        load.start()

    def peer(step):
        j = lax.rem(me + step, devices)
        je, jt = j // tensors, lax.rem(j, tensors)
        return j, je, {"expert": je, "tensor": jt}

    barrier = pltpu.get_barrier_semaphore()

    @pl.loop(1, devices)
    def _(step):
        pl.semaphore_signal(barrier, inc=1, device_id=peer(step)[2], device_id_type=MESH)

    row_slot = lax.broadcasted_iota(jnp.int32, (rows, slots), 0) // images
    col_slot = lax.broadcasted_iota(jnp.int32, (rows, slots), 1)
    spread = jnp.where(row_slot == col_slot, 1.0, 0.0).astype(jnp.bfloat16)
    keys_t = jnp.dot(spread, keys_ref[...], preferred_element_type=jnp.float32)
    key_inv = lax.rsqrt(jnp.sum(keys_t * keys_t, axis=1, keepdims=True) + EPS)
    key_gain = key_inv * scale_ref[0]
    keys_b = keys_t.astype(jnp.bfloat16)

    loads[0].wait()
    flat = tok[...].reshape(images * seq, width)
    raw = lax.dot_general(keys_b, flat, NT, preferred_element_type=jnp.float32)
    part = jnp.zeros((images * seq, 128), jnp.float32)
    for c in range(width // 128):
        piece = flat[:, c * 128:(c + 1) * 128].astype(jnp.float32)
        part = part + piece * piece
    row_sq = lax.dot_general(
        jnp.ones((8, 128), jnp.float32), part, NT,
        precision=lax.Precision.HIGHEST, preferred_element_type=jnp.float32,
    )[0:1]
    logits = key_gain * lax.rsqrt(row_sq + EPS) * raw
    row_image = lax.broadcasted_iota(jnp.int32, logits.shape, 0) % images
    col_image = lax.broadcasted_iota(jnp.int32, logits.shape, 1) // seq
    expo = jnp.where(row_image == col_image, jnp.exp(logits), 0.0)
    dispatch = (expo / jnp.sum(expo, axis=1, keepdims=True)).astype(jnp.bfloat16)
    slot_in = jnp.dot(dispatch, flat, preferred_element_type=jnp.float32).astype(jnp.bfloat16)
    for s in range(slots):
        send1[s] = slot_in[s * images:(s + 1) * images]

    pl.semaphore_wait(barrier, devices - 1)

    own = pltpu.make_async_copy(send1.at[e], recv1.at[me], recv_sem1)
    own.start()

    @pl.loop(1, devices)
    def _(step):
        _, je, device = peer(step)
        pltpu.make_async_remote_copy(
            src_ref=send1.at[je], dst_ref=recv1.at[me], send_sem=send_sem1, recv_sem=recv_sem1,
            device_id=device, device_id_type=MESH,
        ).start()

    combine = expo / jnp.sum(expo, axis=0, keepdims=True)
    comb[...] = jnp.concatenate([combine] * tensors, axis=0).T.astype(jnp.bfloat16)

    loads[1].wait()
    pltpu.make_async_copy(recv1, recv1, recv_sem1).wait()
    x = recv1[...].reshape(devices * images, width)
    half = w_in.shape[1]
    for c in range(0, half, 256):
        size = min(256, half - c)
        pre = jnp.dot(x, w_in[:, c:c + size], preferred_element_type=jnp.float32)
        pre = pre + b_in_ref[:, c:c + size].astype(jnp.float32)
        hidden[:, c:c + size] = jax.nn.gelu(pre).astype(jnp.bfloat16)

    loads[2].wait()
    h = hidden[...]
    first_half = jnp.where(t == 0, 1.0, 0.0)
    for c, (start, size) in enumerate(cuts):
        y = jnp.dot(h, w_out[:, start:start + size], preferred_element_type=jnp.float32)
        y = y + b_out_ref[:, start:start + size].astype(jnp.float32) * first_half
        y = y.astype(jnp.bfloat16)
        send2[c][...] = y.reshape(devices, images, size)
        pltpu.make_async_copy(send2[c].at[me], recv2[c].at[home], recv_sem2.at[c]).start()

        @pl.loop(1, devices)
        def _(step):
            j, _, device = peer(step)
            pltpu.make_async_remote_copy(
                src_ref=send2[c].at[j], dst_ref=recv2[c].at[home],
                send_sem=send_sem2.at[c], recv_sem=recv_sem2.at[c],
                device_id=device, device_id_type=MESH,
            ).start()

    cm = comb[...]
    for c, (start, size) in enumerate(cuts):
        pltpu.make_async_copy(recv2[c], recv2[c], recv_sem2.at[c]).wait()
        mixed = jnp.dot(cm, recv2[c][...].reshape(devices * images, size), preferred_element_type=jnp.float32)
        out_ref[:, :, start:start + size] = mixed.astype(jnp.bfloat16).reshape(images, seq, size)

    first = recv1.at[pl.ds(0, devices - 1)]
    pltpu.make_async_copy(first, first, send_sem1).wait()
    for c in range(n_cut):
        block = recv2[c].at[pl.ds(0, devices - 1)]
        pltpu.make_async_copy(block, block, send_sem2.at[c]).wait()


def local(experts, tensors, tokens, slot_keys, logit_scale, w_in, b_in, w_out, b_out):
    images, seq, width = tokens.shape
    slots = slot_keys.shape[1]
    half = w_in.shape[2]
    devices = experts * tensors
    cuts = [(0, width)]
    bf16 = jnp.bfloat16
    return pl.pallas_call(
        functools.partial(kernel, experts, tensors, cuts),
        out_shape=pltpu.VMEM(tokens.shape, bf16),
        in_specs=[
            pl.BlockSpec(memory_space=pltpu.HBM),
            pl.BlockSpec(memory_space=pltpu.VMEM),
            pl.BlockSpec(memory_space=pltpu.SMEM),
            pl.BlockSpec(memory_space=pltpu.HBM),
            pl.BlockSpec(memory_space=pltpu.VMEM),
            pl.BlockSpec(memory_space=pltpu.HBM),
            pl.BlockSpec(memory_space=pltpu.VMEM),
        ],
        out_specs=pl.BlockSpec(memory_space=pltpu.VMEM),
        scratch_shapes=[
            pltpu.VMEM((images, seq, width), bf16),
            pltpu.VMEM((width, half), bf16),
            pltpu.VMEM((half, width), bf16),
            pltpu.VMEM((slots, images, width), bf16),
            pltpu.VMEM((devices, images, width), bf16),
            pltpu.VMEM((devices * images, width), bf16),
            pltpu.VMEM((devices * images, half), bf16),
            pltpu.VMEM((images * seq, tensors * slots * images), bf16),
            *[pltpu.VMEM((devices, images, size), bf16) for _, size in cuts],
            *[pltpu.VMEM((devices, images, size), bf16) for _, size in cuts],
            pltpu.SemaphoreType.DMA((3,)),
            pltpu.SemaphoreType.DMA,
            pltpu.SemaphoreType.DMA,
            pltpu.SemaphoreType.DMA((len(cuts),)),
            pltpu.SemaphoreType.DMA((len(cuts),)),
        ],
        compiler_params=pltpu.CompilerParams(collective_id=0, has_side_effects=True, vmem_limit_bytes=61 * 2**20),
    )(tokens, slot_keys.T, logit_scale.reshape(1), w_in, b_in, w_out, b_out)


def solution(mesh):
    placed = (
        P(("expert", "tensor"), None, None),
        P(),
        P(),
        P("expert", None, "tensor"),
        P("expert", "tensor"),
        P("expert", "tensor", None),
        P("expert", None),
    )
    return jax.shard_map(
        functools.partial(local, mesh.shape["expert"], mesh.shape["tensor"]),
        mesh=mesh,
        in_specs=placed,
        out_specs=P(("expert", "tensor"), None, None),
        check_vma=False,
    )
```
